32 devices in a mesh: ep: 8 (over z, x), tp: 4 (over y, core).
Axes of the slice: x: 2, y: 2, z: 4, core: 2. Of those that a mesh axis runs over, the one named last changes fastest.
Arguments:
- tokens: bfloat16 [2048, 2048], P('ep', 'tp'), may hold values from -180 to 180
- norm_gain: float32 [2048], replicated, may hold values from 0.1 to 1.9
- router_weight: bfloat16 [2048, 60], P('tp'), may hold values from -2 to 2
- shared_gate_w: bfloat16 [2048], replicated, may hold values from -0.125 to 0.125
- expert_ids: int32 [2048, 4], P('ep'), may hold values from 0 to 59, all different within a row; in each aligned block of 256 rows (0 to 255, 256 to 511, ...) at most 32 rows name the same one
- w_gate: bfloat16 [64, 2048, 1408], P('ep', None, 'tp'), may hold values from -0.125 to 0.125
- w_up: bfloat16 [64, 2048, 1408], P('ep', None, 'tp'), may hold values from -0.125 to 0.125
- w_down: bfloat16 [64, 1408, 2048], P('ep', 'tp'), may hold values from -1.5 to 1.5
- shared_w_gate: bfloat16 [2048, 2816], P(None, 'tp'), may hold values from -0.125 to 0.125
- shared_w_up: bfloat16 [2048, 2816], P(None, 'tp'), may hold values from -0.125 to 0.125
- shared_w_down: bfloat16 [2816, 2048], P('tp'), may hold values from -0.109375 to 0.109375
Outputs:
- moe_out: bfloat16 [2048, 2048], P('ep', 'tp')
The draws below stay inside these ranges and needn't reach their ends.
Inputs may be any that keep to these rules, and one draw needn't show every extreme that they name: `expert_ids`: each row names 4 different experts below 60. Within the 256 rows of one index of ep no expert is named by more than 32 rows, and in some of these blocks one expert is named by exactly 32 rows.
All inputs are finite; a program needn't handle non-finite values.
Results may differ from the reference program's by a relative error of at most 0.0069.
Values may be sent and summed in bfloat16 or wider, within the bound.
A program may use at most 128 MiB of HBM per device.

```python
import math
import jax
import jax.numpy as jnp
import numpy as np
from jax import lax

D = 2048
FE = 1408
EXPERTS = 60
TOPK = 4
SF = 2816
TOK_DEV = 256
CAP = 32
SLOTS = 64
TOKENS = 2048
N_EP = 8


def draw_tokens(key, part):
    base = jax.random.fold_in(key, 11)
    first, second = jax.random.split(base, 2)
    noise = jnp.clip(jax.random.normal(first, (TOKENS, D), jnp.float32), -4.0, 4.0)
    rising = 3.0 ** (jnp.arange(D, dtype=jnp.float32) / D)
    column = jnp.exp(jax.random.uniform(second, (D,), jnp.float32, math.log(0.3), 0.0)) * rising
    values = noise * column[None, :]
    return values.astype(jnp.bfloat16)


def draw_router_weight(key, part):
    base = jax.random.fold_in(key, 13)
    values = jnp.clip(jax.random.normal(base, (D, EXPERTS), jnp.float32), -4.0, 4.0) * (0.4 / math.sqrt(D))
    values = jnp.clip(values, -2.0, 2.0)
    return values.astype(jnp.bfloat16)


def block_levels(key, extent, cuts, low, largest):
    loudness, own = 1.0, jax.random.fold_in(key, 6)
    for dim, shards_of in cuts:
        steps = jnp.exp(jax.random.uniform(jax.random.fold_in(own, dim), (shards_of,), jnp.float32, low / len(cuts), largest / len(cuts)))
        loudness = loudness * jnp.repeat(steps, extent[dim] // shards_of).reshape([-1 if axis == dim else 1 for axis in range(len(extent))])
    return loudness


def deal_out(own_key, own, number, rows, amount, top, most, slope):
    sequence = jax.random.permutation(own_key, amount)
    packed, ordinary = load_shares(amount, rows * top, most, slope, True), load_shares(amount, rows * top, most, slope, False)
    places = jnp.arange(amount)

    def named(lengths, rotation):
        used = int((lengths > 0).sum())
        fixed = max(1, used // 4)
        shifted = fixed + (places - fixed + rotation * (used - fixed)) % max(1, amount - fixed)
        return jnp.zeros((amount,), jnp.int32).at[sequence[jnp.where(places < fixed, places, shifted)]].set(jnp.asarray(lengths, jnp.int32))

    lengths = jnp.where(number % 4 == 0, named(packed, number // 4), named(ordinary, number - number // 4 - 1))
    mixed = jax.random.permutation(jax.random.fold_in(own, 3), amount)
    giver, receiver = mixed[0:amount // 2 * 2:2], mixed[1:amount // 2 * 2:2]
    slack = jnp.minimum(lengths[giver] - 1, most - lengths[receiver]) // 2
    slack = jnp.where((giver == sequence[0]) | (receiver == sequence[0]) | (lengths[receiver] == 0), 0, jnp.maximum(slack, 0))
    shifted = jax.random.randint(jax.random.fold_in(own, 4), (amount // 2,), 0, 1 << 20) % (slack + 1)
    lengths = lengths.at[giver].add(-shifted).at[receiver].add(shifted)
    members = jnp.searchsorted(jnp.cumsum(lengths), jnp.arange(rows * top), side="right").astype(jnp.int32)
    table = members.reshape(top, rows).T
    table = table[jax.random.permutation(jax.random.fold_in(own, 1), rows)]
    rotation = jax.random.randint(jax.random.fold_in(own, 2), (rows, 1), 0, top)
    return jnp.take_along_axis(table, (jnp.arange(top)[None, :] + rotation) % top, axis=1)


def load_shares(amount, total, most, lean, full):
    weights = [(1 << 20) // math.isqrt(rank ** lean) + 1 for rank in range(1, amount + 1)]
    largest = most if full else min(most, max(-(-total // amount), total * weights[0] // sum(weights)))
    least = 1 if total - largest >= amount - 1 else 0
    given, rest = [largest] + [least] * (amount - 1), total - largest - least * (amount - 1)
    while rest > 0:
        free = [i for i in range(1, amount) if given[i] < largest] or [i for i in range(1, amount) if given[i] < most]
        mass, budget = sum([weights[i] for i in free]), rest
        for i in free:
            extra = min(most - given[i], max(1, budget * weights[i] // mass), rest)
            given[i] = given[i] + extra
            rest = rest - extra
    return np.array(given)


def centred(key, shape, scale, reach, cuts=(), kind=jnp.bfloat16):
    values = jax.random.normal(key, shape, jnp.float32) * scale
    if len(cuts) > 0:
        values = block_levels(key, shape, cuts, -0.22, 0.18) * values
    return jnp.clip(values, min=-reach, max=reach).astype(kind)


def setup_inputs(seed: int = 0) -> dict:
    key_list = jax.random.split(jax.random.key(seed), 12)
    tokens = draw_tokens(jax.random.fold_in(key_list[11], 71), 0)
    norm_gain = jnp.clip(1.0 + 0.18 * jax.random.normal(key_list[1], (D,), jnp.float32), 0.1, 1.9)
    router_weight = draw_router_weight(jax.random.fold_in(key_list[11], 71), 0)
    shared_gate_w = centred(key_list[3], (D,), D ** -0.5, 0.125)
    expert_ids_keys = jax.random.split(jax.random.fold_in(key_list[4], 1), TOKENS // TOK_DEV)
    expert_ids_turns = jax.random.permutation(jax.random.fold_in(key_list[4], 3), TOKENS // TOK_DEV)
    expert_ids = jax.vmap(lambda own, number: deal_out(jax.random.fold_in(key_list[4], 2), own, number, TOK_DEV, EXPERTS, TOPK, CAP, 2))(expert_ids_keys, expert_ids_turns).reshape((TOKENS, TOPK))
    w_gate = centred(key_list[5], (SLOTS, D, FE), D ** -0.5, 0.125, ((0, 8), (2, 4)))
    w_up = centred(key_list[6], (SLOTS, D, FE), D ** -0.5, 0.125, ((0, 8), (2, 4)))
    w_down = centred(key_list[7], (SLOTS, FE, D), 0.25, 1.5, ((0, 8), (1, 4)))
    shared_w_gate = centred(key_list[8], (D, SF), D ** -0.5, 0.125, ((1, 4),))
    shared_w_up = centred(key_list[9], (D, SF), D ** -0.5, 0.125, ((1, 4),))
    shared_w_down = centred(key_list[10], (SF, D), SF ** -0.5, 0.109375, ((0, 4),))
    return {"tokens": tokens, "norm_gain": norm_gain, "router_weight": router_weight, "shared_gate_w": shared_gate_w, "expert_ids": expert_ids, "w_gate": w_gate, "w_up": w_up, "w_down": w_down, "shared_w_gate": shared_w_gate, "shared_w_up": shared_w_up, "shared_w_down": shared_w_down}


def reference(tokens, norm_gain, router_weight, shared_gate_w, expert_ids, w_gate, w_up, w_down, shared_w_gate, shared_w_up, shared_w_down):
    values = tokens.astype(jnp.float32)
    inv_rms = lax.rsqrt(lax.optimization_barrier(jnp.mean(values * values, axis=-1, keepdims=True)) + 1e-06)
    normed = (values * inv_rms * norm_gain[None, :]).astype(jnp.bfloat16)
    logits = jnp.dot(normed, router_weight, preferred_element_type=jnp.float32)
    probs = jax.nn.softmax(logits, axis=-1)
    route_weight = jnp.take_along_axis(probs, expert_ids, axis=1)
    shared_gate_act = jnp.dot(normed, shared_w_gate, preferred_element_type=jnp.float32)
    shared_up_act = jnp.dot(normed, shared_w_up, preferred_element_type=jnp.float32)
    shared_hidden = (jax.nn.silu(shared_gate_act) * shared_up_act).astype(jnp.bfloat16)
    shared = jnp.dot(shared_hidden, shared_w_down, preferred_element_type=jnp.float32)
    share_gate = jax.nn.sigmoid(jnp.dot(normed, shared_gate_w, preferred_element_type=jnp.float32))
    assigns = TOKENS * TOPK
    blocked = expert_ids.reshape(N_EP, TOK_DEV * TOPK)
    one_hot = (blocked[:, :, None] == jnp.arange(EXPERTS, dtype=jnp.int32)[None, None, :]).astype(jnp.int32)
    before = jnp.cumsum(one_hot, axis=1) - one_hot
    order_rank = lax.optimization_barrier(jnp.sum(before * one_hot, axis=-1))
    position = jnp.arange(N_EP, dtype=jnp.int32)[:, None] * CAP + order_rank
    assign_ids = jnp.arange(assigns, dtype=jnp.int32)
    table = jnp.full((EXPERTS, N_EP * CAP), assigns, jnp.int32)
    table = table.at[blocked.reshape(-1), position.reshape(-1)].set(assign_ids)
    normed_pad = jnp.concatenate([normed, jnp.zeros((1, D), jnp.bfloat16)], axis=0)
    weight_pad = jnp.concatenate([route_weight.reshape(-1), jnp.zeros((1,), jnp.float32)], axis=0)

    def expert_step(total, expert):
        entries = table[expert]
        token_ids = (entries // TOPK).astype(jnp.int32)
        rows = normed_pad[token_ids]
        gate_act = jnp.dot(rows, w_gate[expert], preferred_element_type=jnp.float32)
        up_act = jnp.dot(rows, w_up[expert], preferred_element_type=jnp.float32)
        hidden = (jax.nn.silu(gate_act) * up_act).astype(jnp.bfloat16)
        result = jnp.dot(hidden, w_down[expert], preferred_element_type=jnp.float32).astype(jnp.bfloat16)
        total = total.at[token_ids].add(weight_pad[entries][:, None] * result.astype(jnp.float32))
        return (total, None)
    routed, _ = lax.scan(expert_step, jnp.zeros((TOKENS + 1, D), jnp.float32), jnp.arange(EXPERTS, dtype=jnp.int32))
    return (share_gate[:, None] * shared + routed[:TOKENS]).astype(jnp.bfloat16)
```

```python
import jax
import jax.numpy as jnp
from jax import lax
from jax.sharding import PartitionSpec as P

F32 = jnp.float32
BF16 = jnp.bfloat16


def send_back(summed):
    return lax.all_to_all(summed, "ep", split_axis=0, concat_axis=0, tiled=True)


def expert_rows(arrived, w_gate, w_up, w_down):
    gate_act = jnp.einsum("sekd,edf->sekf", arrived, w_gate, preferred_element_type=jnp.float32)
    up_act = jnp.einsum("sekd,edf->sekf", arrived, w_up, preferred_element_type=jnp.float32)
    hidden = (jax.nn.silu(gate_act) * up_act).astype(jnp.bfloat16)
    partial_out = jnp.einsum("sekf,efd->sekd", hidden, w_down, preferred_element_type=jnp.float32)
    summed = lax.psum_scatter(partial_out, "tp", scatter_dimension=3, tiled=True).astype(
        jnp.bfloat16
    )
    return send_back(summed)


def sliced_rows(arrived, w_gate, w_up, w_down):
    complete = lax.all_gather(arrived, "tp", axis=3, tiled=True)
    return expert_rows(complete, w_gate, w_up, w_down)


def dispatch_plan(
    tokens,
    norm_gain,
    router_weight,
    shared_gate_w,
    expert_ids,
    w_gate,
    w_up,
    w_down,
    shared_w_gate,
    shared_w_up,
    shared_w_down,
):
    width = tokens.shape[1]
    tok_rows = tokens.shape[0]
    column_start = lax.axis_index("tp") * width
    whole = lax.all_gather(tokens, "tp", axis=1, tiled=True)
    values = whole.astype(jnp.float32)
    inv_rms = lax.rsqrt(jnp.mean(values * values, axis=-1, keepdims=True) + 1e-06)
    normed = (values * inv_rms * norm_gain[None, :]).astype(jnp.bfloat16)
    own_part = lax.dynamic_slice_in_dim(normed, column_start, width, 1)
    partial_logits = jnp.dot(own_part, router_weight, preferred_element_type=jnp.float32)
    logits = lax.psum(partial_logits, "tp")
    probs = jax.nn.softmax(logits, axis=-1)
    expert_count = logits.shape[1]
    matches = expert_ids[:, :, None] == jnp.arange(expert_count, dtype=jnp.int32)[None, None, :]
    route_weight = jnp.sum(jnp.where(matches, probs[:, None, :], 0.0), axis=-1)
    gate_whole, up_whole, down_whole = (w_gate, w_up, w_down)
    experts_here = w_gate.shape[0]
    slot_count = lax.axis_size("ep") * experts_here
    capacity = tok_rows // 8
    flat_ids = expert_ids.reshape(-1)
    one_hot = (flat_ids[:, None] == jnp.arange(slot_count, dtype=jnp.int32)[None, :]).astype(
        jnp.int32
    )
    before = jnp.cumsum(one_hot, axis=0) - one_hot
    order_rank = jnp.sum(before * one_hot, axis=1)
    slot_ids = (flat_ids * capacity + order_rank).reshape(expert_ids.shape)
    targets = jnp.arange(slot_count * capacity, dtype=jnp.int32)
    dispatch_map = jnp.sum(
        (slot_ids[None, :, :] == targets[:, None, None]).astype(jnp.bfloat16), axis=2
    )
    outgoing = jnp.dot(dispatch_map, own_part, preferred_element_type=jnp.float32).astype(
        jnp.bfloat16
    )
    outgoing = outgoing.reshape(lax.axis_size("ep"), experts_here, capacity, width)
    returned = sliced_rows(
        lax.all_to_all(outgoing, "ep", split_axis=0, concat_axis=0, tiled=True),
        w_gate=gate_whole,
        w_up=up_whole,
        w_down=down_whole,
    )
    picked = returned.reshape(slot_count * capacity, width)[slot_ids]
    routed = jnp.sum(route_weight[:, :, None] * picked.astype(jnp.float32), axis=1)
    shared_gate_act = jnp.dot(normed, shared_w_gate, preferred_element_type=jnp.float32)
    shared_up_act = jnp.dot(normed, shared_w_up, preferred_element_type=jnp.float32)
    shared_hidden = (jax.nn.silu(shared_gate_act) * shared_up_act).astype(jnp.bfloat16)
    shared_part = jnp.dot(shared_hidden, shared_w_down, preferred_element_type=jnp.float32)
    shared_own = lax.psum_scatter(shared_part, "tp", scatter_dimension=1, tiled=True)
    share_gate = jax.nn.sigmoid(jnp.dot(normed, shared_gate_w, preferred_element_type=jnp.float32))
    return (share_gate[:, None] * shared_own + routed).astype(jnp.bfloat16)


def gather_plan(
    tokens,
    norm_gain,
    router_weight,
    shared_gate_w,
    expert_ids,
    w_gate,
    w_up,
    w_down,
    shared_w_gate,
    shared_w_up,
    shared_w_down,
):
    rows, width = tokens.shape
    n_ep = lax.axis_size("ep")
    n_tp = lax.axis_size("tp")
    full = n_tp * width
    here = w_gate.shape[0]
    cap = rows // 8
    me = lax.axis_index("ep")

    every = lax.all_gather(tokens, ("ep", "tp"), axis=0)
    ids = lax.all_gather(expert_ids, "ep", axis=0)
    router = lax.all_gather(router_weight, "tp", axis=0, tiled=True)

    whole = every.reshape(n_ep, n_tp, rows, width).transpose(0, 2, 1, 3)
    values = whole.reshape(n_ep, rows, full).astype(F32)
    inv_rms = lax.rsqrt(jnp.mean(values * values, axis=-1, keepdims=True) + 1e-06)
    normed = (values * inv_rms * norm_gain).astype(BF16)

    logits = jnp.einsum("std,dx->stx", normed, router, preferred_element_type=F32)
    probs = jax.nn.softmax(logits, axis=-1)
    probs = jnp.pad(probs, ((0, 0), (0, 0), (0, n_ep * here - probs.shape[-1])))
    local = lax.dynamic_slice_in_dim(probs, me * here, here, 2)
    names = me * here + jnp.arange(here, dtype=jnp.int32)
    match = jnp.any(ids[:, :, :, None] == names, axis=2)
    lower = jnp.tril(jnp.ones((rows, rows), BF16), -1)
    rank = jnp.einsum("tu,suj->sjt", lower, match.astype(BF16), preferred_element_type=F32)
    match_t = match.transpose(0, 2, 1)
    spot = jnp.where(match_t, rank, -1.0).astype(jnp.int32)
    pick = spot[:, :, None, :] == jnp.arange(cap, dtype=jnp.int32)[None, None, :, None]
    slot_w = jnp.sum(jnp.where(pick, local.transpose(0, 2, 1)[:, :, None, :], 0.0), axis=-1)
    pick = pick.astype(BF16)

    x = jnp.einsum("sjkt,std->jskd", pick, normed, preferred_element_type=F32).astype(BF16)
    gate = jnp.einsum("jskd,jdf->jskf", x, w_gate, preferred_element_type=F32)
    up = jnp.einsum("jskd,jdf->jskf", x, w_up, preferred_element_type=F32)
    hidden = (jax.nn.silu(gate) * up).astype(BF16)
    y = jnp.einsum("jskf,jfd->jskd", hidden, w_down, preferred_element_type=F32)
    y = (y * slot_w.transpose(1, 0, 2)[..., None]).astype(BF16)
    routed = jnp.einsum("sjkt,jskd->std", pick, y, preferred_element_type=F32)

    own = lax.dynamic_index_in_dim(normed, me, 0, keepdims=False)
    sg = jnp.dot(own, shared_w_gate, preferred_element_type=F32)
    su = jnp.dot(own, shared_w_up, preferred_element_type=F32)
    sh = (jax.nn.silu(sg) * su).astype(BF16)
    part = jnp.dot(sh, shared_w_down, preferred_element_type=F32)
    share = jax.nn.sigmoid(jnp.dot(own, shared_gate_w, preferred_element_type=F32))
    part = share[:, None] * part
    mine = (jnp.arange(n_ep) == me)[:, None, None]
    total = (routed + jnp.where(mine, part[None], 0.0)).astype(BF16)
    total = total.reshape(n_ep, rows, n_tp, width)
    total = lax.psum_scatter(total, "tp", scatter_dimension=2, tiled=True)
    total = total.reshape(n_ep * rows, width)
    return lax.psum_scatter(total, "ep", scatter_dimension=0, tiled=True)


def solution(mesh):
    def per_device(tokens, *rest):
        gathered = mesh.size * tokens.size * tokens.dtype.itemsize
        plan = gather_plan if gathered <= 16 << 20 else dispatch_plan
        return plan(tokens, *rest)

    return jax.shard_map(
        per_device,
        mesh=mesh,
        in_specs=(
            P("ep", "tp"),
            P(),
            P("tp", None),
            P(),
            P("ep", None),
            P("ep", None, "tp"),
            P("ep", None, "tp"),
            P("ep", "tp", None),
            P(None, "tp"),
            P(None, "tp"),
            P("tp", None),
        ),
        out_specs=P("ep", "tp"),
        check_vma=False,
    )
```
